32 devices in a mesh: tok: 8 (over z, x), exp: 4 (over y, core).
Axes of the slice: x: 2, y: 2, z: 4, core: 2. Of those that a mesh axis runs over, the one named last changes fastest.
Arguments:
- tokens: bfloat16 [16384, 7168], P('tok', 'exp'), may hold values from -6 to 6
- gate_weight: bfloat16 [7168, 256], P('exp'), may hold values from -0.0625 to 0.0625
- expert_ids: int32 [16384, 8], P('tok'), may hold values from 0 to 255, all different within a row
- expert_bias: float32 [256], P('exp'), may hold values from -0.002 to 0.002
Outputs:
- affinities: float32 [16384, 256], P('tok', 'exp')
- weights: float32 [16384, 8], P('tok')
- load: float32 [256], replicated
- new_bias: float32 [256], replicated
The draws below stay inside these ranges and needn't reach their ends.
All inputs are finite; a program needn't handle non-finite values.
Results may differ from the reference program's by a relative error of at most 0.0003.
Values may be sent and summed in bfloat16 or wider, within the bound.
No kernel may reach another device: no remote copies, remote signals or barrier semaphores. Data moves between devices by JAX's collectives and lax.ppermute only.
A program may use at most 64 MiB of HBM per device.

```python
import jax
import jax.numpy as jnp
from jax import lax

D = 7168
E = 256
TOPK = 8
TOKENS = 16384


def block_scale(rng, extent, shards, low, high):
    def one(axis_at, blocks):
        draws = jax.random.uniform(jax.random.fold_in(jax.random.fold_in(rng, 6), axis_at), (blocks,), jnp.float32, low / len(shards), high / len(shards))
        return jnp.repeat(jnp.exp(draws), extent[axis_at] // blocks).reshape((-1,) + (1,) * (len(extent) - axis_at - 1))

    loudness = one(*shards[0])
    for cut in shards[1:]:
        loudness = loudness * one(*cut)
    return loudness


def picks_of(stream_key, rows, count, top, lift):
    ranking = jax.random.permutation(jax.random.fold_in(stream_key, 1), count)
    boost = ranking
    for power in range(3):
        boost = boost * boost // count
    boost = boost * lift // count
    tickets = jax.random.randint(jax.random.fold_in(stream_key, 2), (rows, count), 0, 4096) + boost
    holders = jax.random.permutation(jax.random.fold_in(stream_key, 3), rows)[jnp.arange(count) % rows]
    tickets = jnp.where(jnp.arange(rows)[:, None] == holders[None, :], 1 << 14, tickets)
    priority = tickets * count + jnp.arange(count)
    return lax.top_k(priority.astype(jnp.int32), top)[1].astype(jnp.int32)


def gaussian(own_key, shape, deviation, bound, shards=(), kind=jnp.bfloat16):
    loudness = block_scale(own_key, shape, shards, -0.22, 0.18) if shards else 1.0
    values = jax.random.normal(own_key, shape, jnp.float32) * deviation * loudness
    return jnp.minimum(jnp.maximum(values, -bound), bound).astype(kind)


def setup_inputs(seed: int = 0) -> dict:
    key_of = jax.random.split(jax.random.key(seed), 5)
    tokens = gaussian(key_of[0], (TOKENS, D), 1.0, 6.0, ((0, 8), (1, 4)))
    gate_weight = gaussian(key_of[1], (D, E), D ** -0.5, 0.0625, ((0, 4),))
    expert_ids = picks_of(key_of[2], TOKENS, E, TOPK, 512)
    expert_bias = jnp.clip(jax.random.uniform(key_of[3], (E,), jnp.float32, -0.002, 0.002) * block_scale(key_of[3], (E,), ((0, 4),), -0.4, 0.0), -0.002, 0.002)
    return {"tokens": tokens, "gate_weight": gate_weight, "expert_ids": expert_ids, "expert_bias": expert_bias}


def reference(tokens, gate_weight, expert_ids, expert_bias):
    logits = jnp.dot(tokens, gate_weight, preferred_element_type=jnp.float32)
    affinities = jax.nn.sigmoid(logits)
    chosen = jnp.take_along_axis(affinities, expert_ids, axis=1)
    weights = 2.5 * chosen / jnp.sum(chosen, axis=1, keepdims=True)
    numbers = jnp.arange(E, dtype=jnp.int32)
    load = jnp.sum((expert_ids[:, :, None] == numbers[None, None, :]).astype(jnp.float32), axis=(0, 1))
    target = jnp.float32(TOKENS * TOPK)
    new_bias = expert_bias + 0.001 * jnp.sign(target - jnp.float32(E) * load)
    return affinities, weights, load, new_bias
```

```python
import jax
import jax.numpy as jnp
from jax import lax
from jax.experimental import pallas as pl
from jax.experimental.pallas import tpu as pltpu
from jax.sharding import PartitionSpec as P

CHUNKS = 2
TILE = 256
LANES = 128
SUBLANES = 8


def swap(value, axis, bit):
    count = lax.axis_size(axis)
    return lax.ppermute(value, axis, [(at, at ^ bit) for at in range(count)])


def bits_of(axis):
    count = lax.axis_size(axis)
    bits = [1 << power for power in range(count.bit_length() - 1)]
    assert 1 << len(bits) == count
    return bits


def partial_logits(tokens, gate_weight, ids_t, chunk, own):
    rows, features = tokens.shape
    experts = gate_weight.shape[1]
    picks = ids_t.shape[0]
    parts = lax.axis_size("exp")
    width = experts // parts
    length = rows // CHUNKS
    tile = min(TILE, length)
    steps = length // tile
    half = experts // 2 + picks

    def body(own_ref, tok_ref, gate_ref, ids_ref, keep_ref, send_ref, turned):
        acc = jnp.dot(tok_ref[...], gate_ref[...], preferred_element_type=jnp.float32)
        turned[...] = acc.T
        me = own_ref[0]
        for block in range(parts):
            start = pl.multiple_of((me ^ block) * width, width)
            target = send_ref if block & 1 else keep_ref
            target[pl.ds((block // 2) * width, width), :] = turned[pl.ds(start, width), :]
        level = lax.broadcasted_iota(jnp.int32, (SUBLANES, LANES), 0)
        for lane in range(0, tile, LANES):
            span = pl.ds(lane, LANES)
            offset = [jnp.broadcast_to(ids_ref[pick:pick + 1, span], (SUBLANES, LANES)) - level for pick in range(picks)]
            total = [jnp.zeros((SUBLANES, LANES), jnp.float32) for _ in range(picks)]
            for group in range(0, experts, SUBLANES):
                values = turned[pl.ds(group, SUBLANES), span]
                total = [jnp.where(offset[pick] == group, values, total[pick]) for pick in range(picks)]
            chosen = jnp.concatenate([jnp.sum(part, axis=0, keepdims=True) for part in total], axis=0)
            keep_ref[pl.ds(experts // 2, picks), span] = chosen
            send_ref[pl.ds(experts // 2, picks), span] = chosen

    out = jax.ShapeDtypeStruct((half, length), jnp.float32)
    first = chunk * steps
    return pl.pallas_call(
        body,
        out_shape=(out, out),
        grid=(steps,),
        in_specs=[
            pl.BlockSpec(memory_space=pltpu.SMEM),
            pl.BlockSpec((tile, features), lambda i: (first + i, 0)),
            pl.BlockSpec((features, experts), lambda i: (0, 0)),
            pl.BlockSpec((picks, tile), lambda i: (0, first + i)),
        ],
        out_specs=(pl.BlockSpec((half, tile), lambda i: (0, i)), pl.BlockSpec((half, tile), lambda i: (0, i))),
        scratch_shapes=[pltpu.VMEM((experts, tile), jnp.float32)],
        name="partial_logits",
    )(own, tokens, gate_weight, ids_t)


def count_experts(ids_t, experts):
    picks, rows = ids_t.shape

    def body(ids_ref, out_ref, seen):
        level = lax.broadcasted_iota(jnp.int32, (SUBLANES, LANES), 0)
        seen[...] = jnp.zeros_like(seen)

        def block(at, carry):
            span = pl.ds(pl.multiple_of(at * LANES, LANES), LANES)
            offset = [jnp.broadcast_to(ids_ref[pick:pick + 1, span], (SUBLANES, LANES)) - level for pick in range(picks)]
            for group in range(0, experts, SUBLANES):
                hit = offset[0] == group
                for pick in range(1, picks):
                    hit = jnp.logical_or(hit, offset[pick] == group)
                seen[pl.ds(group, SUBLANES), :] += jnp.where(hit, jnp.float32(1.0), jnp.float32(0.0))
            return carry

        lax.fori_loop(0, rows // LANES, block, 0)
        ones = jnp.ones((SUBLANES, LANES), jnp.bfloat16)
        out_ref[...] = lax.dot_general(ones, seen[...].astype(jnp.bfloat16), (((1,), (1,)), ((), ())), preferred_element_type=jnp.float32)

    return pl.pallas_call(
        body,
        out_shape=jax.ShapeDtypeStruct((SUBLANES, experts), jnp.float32),
        scratch_shapes=[pltpu.VMEM((experts, LANES), jnp.float32)],
        name="count_experts",
    )(ids_t)


def local(tokens, gate_weight, expert_ids, expert_bias):
    rows = tokens.shape[0]
    experts = gate_weight.shape[1]
    picks = expert_ids.shape[1]
    width = expert_bias.shape[0]
    own = lax.axis_index("exp").astype(jnp.int32)
    bits = bits_of("exp")
    ids_t = expert_ids.T

    bias = lax.dynamic_update_slice(jnp.zeros((experts,), jnp.float32), expert_bias, (own * width,))
    for bit in bits:
        bias = bias + swap(bias, "exp", bit)

    affinities, weights = [], []
    for chunk in range(CHUNKS):
        keep, send = partial_logits(tokens, gate_weight, ids_t, chunk, own[None])
        total = keep + swap(send, "exp", bits[0])
        for bit in bits[1:]:
            blocks = (total.shape[0] - picks) // width
            own_rows = total[:width * (blocks // 2)]
            other_rows = total[width * (blocks // 2):]
            chosen_rows = total[width * blocks:]
            arrived = swap(other_rows, "exp", bit)
            total = jnp.concatenate([own_rows, chosen_rows], axis=0) + arrived
        affinities.append(jax.nn.sigmoid(total[:width]))
        chosen = jax.nn.sigmoid(total[width:])
        weights.append(2.5 * chosen / jnp.sum(chosen, axis=0, keepdims=True))

    load = count_experts(ids_t, experts)[:1]
    for bit in bits_of("tok"):
        load = load + swap(load, "tok", bit)
    load = load.reshape(experts)
    target = jnp.float32(rows * lax.axis_size("tok") * picks)
    new_bias = bias + 0.001 * jnp.sign(target - jnp.float32(experts) * load)
    return (jnp.concatenate(affinities, axis=1).T, jnp.concatenate(weights, axis=1).T, load, new_bias)


def solution(mesh):
    in_specs = (P("tok", "exp"), P("exp", None), P("tok", None), P("exp"))
    out_specs = (P("tok", "exp"), P("tok", None), P(), P())
    return jax.shard_map(local, mesh=mesh, in_specs=in_specs, out_specs=out_specs, check_vma=False)
```

```python
import jax
import jax.numpy as jnp
from jax import lax
from jax.experimental import pallas as pl
from jax.experimental.pallas import tpu as pltpu
from jax.sharding import PartitionSpec as P

CHUNKS = 2
TILE = 256
LANES = 128
SUBLANES = 8
PER_FEATURE = 6.0 * 0.0625
TOP = 32767.0


def swap(value, axis, bit):
    count = lax.axis_size(axis)
    return lax.ppermute(value, axis, [(at, at ^ bit) for at in range(count)])


def bits_of(axis):
    count = lax.axis_size(axis)
    bits = [1 << power for power in range(count.bit_length() - 1)]
    assert 1 << len(bits) == count
    return bits


def partial_logits(tokens, gate_weight, ids_t, chunk, own):
    rows, features = tokens.shape
    experts = gate_weight.shape[1]
    picks = ids_t.shape[0]
    parts = lax.axis_size("exp")
    width = experts // parts
    length = rows // CHUNKS
    tile = min(TILE, length)
    steps = length // tile
    half = experts // 2 + picks
    first = chunk * length

    def body(own_ref, tok_ref, gate_ref, ids_ref, keep_ref, send_ref, tok_buf, turned_even, turned_odd, sems):
        copies = [pltpu.make_async_copy(tok_ref.at[pl.ds(first + at * tile, tile), :], tok_buf.at[at], sems.at[at]) for at in range(steps)]
        for copy in copies:
            copy.start()
        me = own_ref[0]
        level = lax.broadcasted_iota(jnp.int32, (SUBLANES, LANES), 0)
        turned = (turned_even, turned_odd)

        def finish(at):
            source = turned[at % 2]
            whole = pl.ds(at * tile, tile)
            for block in range(parts):
                start = pl.multiple_of((me ^ block) * width, width)
                target = send_ref if block & 1 else keep_ref
                target[pl.ds((block // 2) * width, width), whole] = source[pl.ds(start, width), :]
            for lane in range(0, tile, LANES):
                span = pl.ds(at * tile + lane, LANES)
                there = pl.ds(first + at * tile + lane, LANES)
                offset = [jnp.broadcast_to(ids_ref[pick:pick + 1, there], (SUBLANES, LANES)) - level for pick in range(picks)]
                total = [jnp.zeros((SUBLANES, LANES), jnp.float32) for _ in range(picks)]
                for group in range(0, experts, SUBLANES):
                    values = source[pl.ds(group, SUBLANES), pl.ds(lane, LANES)]
                    total = [jnp.where(offset[pick] == group, values, total[pick]) for pick in range(picks)]
                chosen = jnp.concatenate([jnp.sum(part, axis=0, keepdims=True) for part in total], axis=0)
                keep_ref[pl.ds(experts // 2, picks), span] = chosen
                send_ref[pl.ds(experts // 2, picks), span] = chosen

        for at in range(steps):
            copies[at].wait()
            acc = jnp.dot(tok_buf[at], gate_ref[...], preferred_element_type=jnp.float32)
            turned[at % 2][...] = acc.T
            if at:
                finish(at - 1)
        finish(steps - 1)

    out = pltpu.VMEM((half, length), jnp.float32)
    return pl.pallas_call(
        body,
        out_shape=(out, out),
        in_specs=[
            pl.BlockSpec(memory_space=pltpu.SMEM),
            pl.BlockSpec(memory_space=pl.ANY),
            pl.BlockSpec(memory_space=pltpu.VMEM),
            pl.BlockSpec(memory_space=pltpu.VMEM),
        ],
        out_specs=(pl.BlockSpec(memory_space=pltpu.VMEM), pl.BlockSpec(memory_space=pltpu.VMEM)),
        scratch_shapes=[
            pltpu.VMEM((steps, tile, features), tokens.dtype),
            pltpu.VMEM((experts, tile), jnp.float32),
            pltpu.VMEM((experts, tile), jnp.float32),
            pltpu.SemaphoreType.DMA((steps,)),
        ],
        name="partial_logits",
    )(own, tokens, gate_weight, ids_t)


def count_experts(ids_t, experts):
    picks, rows = ids_t.shape

    def body(ids_ref, out_ref, seen):
        level = lax.broadcasted_iota(jnp.int32, (SUBLANES, LANES), 0)
        tall = 8
        for group in range(0, experts, SUBLANES * tall):

            def block(at, total):
                span = pl.ds(pl.multiple_of(at * LANES, LANES), LANES)
                offset = [jnp.broadcast_to(ids_ref[pick:pick + 1, span], (SUBLANES, LANES)) - level for pick in range(picks)]
                grown = []
                for add in range(tall):
                    hit = offset[0] == group + add * SUBLANES
                    for pick in range(1, picks):
                        hit = jnp.logical_or(hit, offset[pick] == group + add * SUBLANES)
                    grown.append(total[add] + jnp.where(hit, jnp.float32(1.0), jnp.float32(0.0)))
                return tuple(grown)

            total = lax.fori_loop(0, rows // LANES, block, tuple(jnp.zeros((SUBLANES, LANES), jnp.float32) for _ in range(tall)), unroll=2)
            seen[pl.ds(group, SUBLANES * tall), :] = jnp.concatenate(total, axis=0).astype(jnp.bfloat16)
        ones = jnp.ones((SUBLANES, LANES), jnp.bfloat16)
        out_ref[...] = lax.dot_general(ones, seen[...], (((1,), (1,)), ((), ())), preferred_element_type=jnp.float32)

    return pl.pallas_call(
        body,
        out_shape=pltpu.VMEM((SUBLANES, experts), jnp.float32),
        in_specs=[pl.BlockSpec(memory_space=pltpu.VMEM)],
        out_specs=pl.BlockSpec(memory_space=pltpu.VMEM),
        scratch_shapes=[pltpu.VMEM((experts, LANES), jnp.bfloat16)],
        name="count_experts",
    )(ids_t)


def encode(values, step):
    groups = values.reshape(-1, SUBLANES, values.shape[1])
    size = jnp.ceil(jnp.max(jnp.abs(groups), axis=0) * jnp.float32(1.0 / step)) + 1.0
    codes = jnp.round(groups * (jnp.float32(TOP / step) / size)).astype(jnp.int32)
    whole = size.astype(jnp.int32)[None]
    if codes.shape[0] % 2 == 0:
        whole = jnp.concatenate([whole, whole], axis=0)
    codes = jnp.concatenate([codes, whole], axis=0)
    middle = codes.shape[0] // 2
    packed = (codes[:middle] << 16) | (codes[middle:] & 0xFFFF)
    return packed.reshape(-1, values.shape[1])


def decode(packed, groups, step):
    words = packed.reshape(-1, SUBLANES, packed.shape[1])
    codes = jnp.concatenate([words >> 16, (words << 16) >> 16], axis=0)
    size = (codes[-1] & 0xFFFF).astype(jnp.float32) * jnp.float32(step / TOP)
    return (codes[:groups].astype(jnp.float32) * size).reshape(-1, packed.shape[1])


def local(tokens, gate_weight, expert_ids, expert_bias):
    rows, features = tokens.shape
    experts = gate_weight.shape[1]
    picks = expert_ids.shape[1]
    width = expert_bias.shape[0]
    parts = lax.axis_size("exp")
    own = lax.axis_index("exp").astype(jnp.int32)
    bits = bits_of("exp")
    ids_t = expert_ids.T

    bias = lax.dynamic_update_slice(jnp.zeros((experts,), jnp.float32), expert_bias, (own * width,))
    pairs = [partial_logits(tokens, gate_weight, ids_t, chunk, own[None]) for chunk in range(CHUNKS)]
    totals = [keep + swap(send, "exp", bits[0]) for keep, send in pairs]
    bias = bias + swap(bias, "exp", bits[0])
    step = features * parts * PER_FEATURE / 65000.0
    for bit in bits[1:]:
        sent, mine = [], []
        for total in totals:
            blocks = (total.shape[0] - picks) // width
            near = width * (blocks // 2)
            mine.append(jnp.concatenate([total[:near], total[width * blocks:]], axis=0))
            sent.append(encode(total[near:], step))
        if bit == bits[-1]:
            sent[0], ids_t = lax.optimization_barrier((sent[0], ids_t))
            load = count_experts(ids_t, experts)[:1]
            sent[-1], load, bias = lax.optimization_barrier((sent[-1], load, bias))
        arrived = [swap(packed, "exp", bit) for packed in sent]
        bias = bias + swap(bias, "exp", bit)
        totals = [kept + decode(packed, kept.shape[0] // SUBLANES, step) for kept, packed in zip(mine, arrived)]

    for bit in bits_of("tok"):
        load = load + swap(load, "tok", bit)
    load = load.reshape(experts)
    totals[-1], bias, load = lax.optimization_barrier((totals[-1], bias, load))
    affinities, weights = [], []
    for total in totals:
        affinities.append(jax.nn.sigmoid(total[:width]))
        chosen = jax.nn.sigmoid(total[width:])
        weights.append(2.5 * chosen / jnp.sum(chosen, axis=0, keepdims=True))

    target = jnp.float32(rows * lax.axis_size("tok") * picks)
    new_bias = bias + 0.001 * jnp.sign(target - jnp.float32(experts) * load)
    return (jnp.concatenate(affinities, axis=1).T, jnp.concatenate(weights, axis=1).T, load, new_bias)


def solution(mesh):
    in_specs = (P("tok", "exp"), P("exp", None), P("tok", None), P("exp"))
    out_specs = (P("tok", "exp"), P("tok", None), P(), P())
    return jax.shard_map(local, mesh=mesh, in_specs=in_specs, out_specs=out_specs, check_vma=False)
```
